32 devices in a mesh: data: 32 (over z, y, x, core).
Axes of the slice: x: 2, y: 2, z: 4, core: 2. Of those that a mesh axis runs over, the one named last changes fastest.
Arguments:
- x_step: bfloat16 [2, 64, 576, 768], P(None, 'data')
- labels: int32 [2, 64], P(None, 'data')
- x_next: bfloat16 [64, 576, 768], P('data')
- w_in: float32 [4, 768, 3072], replicated
- w_out: float32 [4, 3072, 768], replicated
- w_head: float32 [768, 1000], replicated
- mom_in: float32 [4, 768, 3072], replicated
- mom_out: float32 [4, 3072, 768], replicated
- mom_head: float32 [768, 1000], replicated
- learn_rate: float32 [], replicated
- mom_coef: float32 [], replicated
Outputs:
- output 1: float32 [64, 1000], P('data')
- output 2: float32 [4, 768, 3072], replicated
- output 3: float32 [4, 3072, 768], replicated
- output 4: float32 [768, 1000], replicated
- output 5: float32 [4, 768, 3072], replicated
- output 6: float32 [4, 3072, 768], replicated
- output 7: float32 [768, 1000], replicated
All inputs are finite; a program needn't handle non-finite values.
Results may differ from the reference program's by a relative error of at most 0.0167193.
Values are sent between devices in bfloat16 or wider.
A program may use at most 1.25 GiB of HBM per device.

```python
import jax
import jax.numpy as jnp
from jax import lax

D = 768
FF = 3072
SEQ = 576
CLASSES = 1000
LAYERS = 4
BATCH_DEV = 2
GROUP = 32
MICRO = 2
BATCH = GROUP * BATCH_DEV
EXAMPLES = MICRO * BATCH
LN_EPS = 1e-6


def setup_inputs(seed: int = 0) -> dict:
    key_list = jax.random.split(jax.random.key(seed), 13)
    img_step = jax.random.normal(key_list[0], (MICRO, BATCH, 1, D), jnp.float32)
    tok_step = jax.random.normal(key_list[1], (MICRO, BATCH, SEQ, D), jnp.float32)
    img_next = jax.random.normal(key_list[2], (BATCH, 1, D), jnp.float32)
    tok_next = jax.random.normal(key_list[3], (BATCH, SEQ, D), jnp.float32)
    labels = jax.random.randint(key_list[4], (MICRO, BATCH), 0, CLASSES, jnp.int32)
    in_scale = D ** -0.5
    out_scale = FF ** -0.5
    mom_rel = 0.3 * EXAMPLES ** -0.5
    return {
        'x_step': (0.8 * img_step + 0.6 * tok_step).astype(jnp.bfloat16),
        'labels': labels,
        'x_next': (0.8 * img_next + 0.6 * tok_next).astype(jnp.bfloat16),
        'w_in': jax.random.normal(key_list[5], (LAYERS, D, FF), jnp.float32) * in_scale,
        'w_out': jax.random.normal(key_list[6], (LAYERS, FF, D), jnp.float32) * out_scale,
        'w_head': jax.random.normal(key_list[7], (D, CLASSES), jnp.float32) * in_scale,
        'mom_in': jax.random.normal(key_list[8], (LAYERS, D, FF), jnp.float32) * (in_scale * mom_rel),
        'mom_out': jax.random.normal(key_list[9], (LAYERS, FF, D), jnp.float32) * (out_scale * mom_rel),
        'mom_head': jax.random.normal(key_list[10], (D, CLASSES), jnp.float32) * (in_scale * mom_rel),
        'learn_rate': jax.random.uniform(key_list[11], (), jnp.float32, 0.1, 0.2) * EXAMPLES ** 0.5,
        'mom_coef': jax.random.uniform(key_list[12], (), jnp.float32, 0.5, 0.9),
    }


def norm_rows(x_f32):
    row_mean = jnp.mean(x_f32, axis=-1, keepdims=True)
    centered = x_f32 - row_mean
    row_var = jnp.mean(centered * centered, axis=-1, keepdims=True)
    return centered * lax.rsqrt(row_var + LN_EPS)


def block_forward(tok_rows, w_one, w_two):
    x_f32 = tok_rows.astype(jnp.float32)
    normed = norm_rows(x_f32).astype(jnp.bfloat16)
    pre_act = jnp.dot(normed, w_one.astype(jnp.bfloat16), preferred_element_type=jnp.float32)
    hidden = jax.nn.gelu(pre_act).astype(jnp.bfloat16)
    mlp_out = jnp.dot(hidden, w_two.astype(jnp.bfloat16), preferred_element_type=jnp.float32)
    return (x_f32 + mlp_out).astype(jnp.bfloat16)


def image_logits(images, w_in, w_out, w_head):
    n_img = images.shape[0]

    def layer_step(tok_rows, weights):
        return block_forward(tok_rows, weights[0], weights[1]), None

    tok_rows, _ = lax.scan(layer_step, images.reshape(n_img * SEQ, D), (w_in, w_out))
    pooled = jnp.mean(tok_rows.reshape(n_img, SEQ, D), axis=1, dtype=jnp.float32)
    return jnp.dot(pooled.astype(jnp.bfloat16), w_head.astype(jnp.bfloat16), preferred_element_type=jnp.float32)


def group_loss(params, images, lab_row):
    logits = image_logits(images, params[0], params[1], params[2])
    log_prob = jax.nn.log_softmax(logits, axis=-1)
    picked = jnp.take_along_axis(log_prob, lab_row[:, None], axis=-1)
    return -jnp.sum(picked) / EXAMPLES


def reference(x_step, labels, x_next, w_in, w_out, w_head, mom_in, mom_out, mom_head, learn_rate, mom_coef):
    params = (w_in, w_out, w_head)
    img_groups = x_step.reshape(MICRO * GROUP, BATCH_DEV, SEQ, D)
    lab_groups = labels.reshape(MICRO * GROUP, BATCH_DEV)
    grad_fn = jax.grad(group_loss)

    def accumulate(grad_sum, group_in):
        part_grad = grad_fn(params, group_in[0], group_in[1])
        return jax.tree.map(jnp.add, grad_sum, part_grad), None

    zero_grads = jax.tree.map(jnp.zeros_like, params)
    grad_sum, _ = lax.scan(accumulate, zero_grads, (img_groups, lab_groups))
    new_mom_in = mom_coef * mom_in + grad_sum[0]
    new_mom_out = mom_coef * mom_out + grad_sum[1]
    new_mom_head = mom_coef * mom_head + grad_sum[2]
    new_w_in = w_in - learn_rate * new_mom_in
    new_w_out = w_out - learn_rate * new_mom_out
    new_w_head = w_head - learn_rate * new_mom_head
    next_groups = x_next.reshape(GROUP, BATCH_DEV, SEQ, D)
    logits = lax.map(lambda images: image_logits(images, new_w_in, new_w_out, new_w_head), next_groups)
    return (logits.reshape(BATCH, CLASSES), new_w_in, new_w_out, new_w_head, new_mom_in, new_mom_out, new_mom_head)
```

```python
import functools
import math

import jax
import jax.numpy as jnp
from jax import lax
from jax.experimental import pallas as pl
from jax.experimental.pallas import tpu as pltpu
from jax.sharding import PartitionSpec as P

BF16 = jnp.bfloat16
F32 = jnp.float32
LN_EPS = 1e-6
C0 = math.sqrt(2.0 / math.pi)
C1 = 0.044715
CHUNK = 512
ROWS = 256
LANES = 256
FWD_TILE = 768
ACT_ROWS = 64
LN_ROWS = 96
MESH = pl.DeviceIdType.MESH
VMEM_LIMIT = 63 * 1024 * 1024


def norm_stats(x_f32):
    row_mean = jnp.mean(x_f32, axis=-1, keepdims=True)
    centered = x_f32 - row_mean
    inv_std = lax.rsqrt(jnp.mean(centered * centered, axis=-1, keepdims=True) + LN_EPS)
    return centered, inv_std


def norm_rows(x_f32):
    centered, inv_std = norm_stats(x_f32)
    return centered * inv_std


def gelu_parts(pre):
    squared = pre * pre
    gate = 0.5 + 0.5 * jnp.tanh(pre * (C0 + (C0 * C1) * squared))
    return squared, gate, pre * gate


def span(index, size):
    return slice(index * size, index * size + size)


def row_loop(total, step, body):
    @pl.loop(0, total // step)
    def _(index):
        body(pl.ds(pl.multiple_of(index * step, step), step))


def dot(a, b):
    return jnp.dot(a, b, preferred_element_type=F32)


def dot_rhs_t(a, b):
    return lax.dot_general(a, b, (((1,), (1,)), ((), ())), preferred_element_type=F32)


def dot_lhs_t(a, b):
    return lax.dot_general(a, b, (((0,), (0,)), ((), ())), preferred_element_type=F32)


def image_sums(x, image):
    rows = lax.broadcasted_iota(jnp.int32, (8, x.shape[0]), 0)
    cols = lax.broadcasted_iota(jnp.int32, (8, x.shape[0]), 1)
    inside = (cols >= rows * image) & (cols < (rows + 1) * image)
    return dot(inside.astype(F32).astype(BF16), x)


def forward_kernel(
    x_hbm, w_in, w_out, hid, slope, w_in_b, w_out_b, x_out, hid_sum, top_sum,
    x, n, acc, pre, sem, *, tokens, image, tile, layers, chunks,
):
    layer, chunk = pl.program_id(0), pl.program_id(1)

    @pl.when((layer == 0) & (chunk == 0))
    def _():
        load = pltpu.make_async_copy(x_hbm, x, sem)
        load.start()
        load.wait()

    w_in_b[...] = w_in[...].astype(BF16)
    w_out_b[...] = w_out[...].astype(BF16)

    def first(i):
        pre[i % 2] = dot(n[span(i, tile), :], w_in_b[...])

    def act(i):
        for j in range(tile // ACT_ROWS):
            rows = span(i * tile // ACT_ROWS + j, ACT_ROWS)
            squared, gate, value = gelu_parts(pre[i % 2, span(j, ACT_ROWS), :])
            hid[rows, :] = value.astype(BF16)
            slope[rows, :] = (gate + (value * (2 * C0 + (6 * C0 * C1) * squared)) * (1.0 - gate)).astype(BF16)

    def second(i, begin):
        rows = span(i, tile)
        part = dot(hid[rows, :], w_out_b[...])
        acc[rows, :] = part if begin else part + acc[rows, :]

    def begin_rows(i):
        for j in range(tile // LN_ROWS):
            rows = span(i * tile // LN_ROWS + j, LN_ROWS)
            n[rows, :] = norm_rows(x[rows, :].astype(F32)).astype(BF16)

    def end_rows(i):
        for j in range(tile // LN_ROWS):
            rows = span(i * tile // LN_ROWS + j, LN_ROWS)
            value = (x[rows, :].astype(F32) + acc[rows, :]).astype(BF16)
            x[rows, :] = value
            x_out[rows, :] = value

    def run(begin, end):
        steps = [begin_rows] * begin + [first, act, functools.partial(second, begin=begin)] + [end_rows] * end
        count = tokens // tile
        for i in range(count + len(steps) - 1):
            for lag, step in enumerate(steps):
                if 0 <= i - lag < count:
                    step(i - lag)

    @pl.when(chunk == 0)
    def _():
        run(True, False)

    @pl.when((chunk > 0) & (chunk < chunks - 1))
    def _():
        run(False, False)

    @pl.when(chunk == chunks - 1)
    def _():
        run(False, True)

    @pl.when(layer == layers - 1)
    def _():
        hid_sum[...] = image_sums(hid[...], image)

        @pl.when(chunk == chunks - 1)
        def _():
            top_sum[...] = image_sums(x[...], image)


def forward(x, w_in, w_out, image=576):
    tokens, dim = x.shape
    layers, _, hidden = w_in.shape
    chunks = hidden // CHUNK
    top = layers - 1
    one = pl.squeezed
    in_spec = pl.BlockSpec((one, dim, CHUNK), lambda l, f: (l, 0, f))
    out_spec = pl.BlockSpec((one, CHUNK, dim), lambda l, f: (l, f, 0))
    act = jax.ShapeDtypeStruct((layers, chunks, tokens, CHUNK), BF16)
    return pl.pallas_call(
        functools.partial(forward_kernel, tokens=tokens, image=image, tile=FWD_TILE, layers=layers, chunks=chunks),
        grid=(layers, chunks),
        in_specs=[pl.BlockSpec(memory_space=pl.ANY), in_spec, out_spec],
        out_specs=[
            pl.BlockSpec((one, one, tokens, CHUNK), lambda l, f: (l, jnp.where(l == top, 0, f), 0, 0)),
            pl.BlockSpec((one, one, tokens, CHUNK), lambda l, f: (l, f, 0, 0)),
            in_spec,
            out_spec,
            pl.BlockSpec((one, tokens, dim), lambda l, f: (l, 0, 0)),
            pl.BlockSpec((one, 8, CHUNK), lambda l, f: (jnp.where(l == top, f, 0), 0, 0)),
            pl.BlockSpec((8, dim), lambda l, f: (0, 0)),
        ],
        out_shape=[
            act,
            act,
            jax.ShapeDtypeStruct(w_in.shape, BF16),
            jax.ShapeDtypeStruct(w_out.shape, BF16),
            jax.ShapeDtypeStruct((layers, tokens, dim), BF16),
            jax.ShapeDtypeStruct((chunks, 8, CHUNK), F32),
            jax.ShapeDtypeStruct((8, dim), F32),
        ],
        scratch_shapes=[
            pltpu.VMEM((tokens, dim), BF16),
            pltpu.VMEM((tokens, dim), BF16),
            pltpu.VMEM((tokens, dim), F32),
            pltpu.VMEM((2, FWD_TILE, CHUNK), F32),
            pltpu.SemaphoreType.DMA,
        ],
        compiler_params=pltpu.CompilerParams(vmem_limit_bytes=VMEM_LIMIT),
        name="forward",
    )(x, w_in, w_out)


PAIRS = 7
STREAM = 4608
HALF = 2304
COLOR = 1152
SIZES = (576, 288, 144)
MASKS = ((2, 8, 4, 16), (4, 8, 2, 16))
READY = (4, 5)
REDUCE = (0, 1, 3, 5, 6, 7, 8)
GATHER = (8, 9, 10, 12, 14, 15)
TICKS = 24
LAST_TICK = READY[1] + 3 * (PAIRS - 1) + GATHER[-1] + 1
GROUPS = 22
EXTRA_TICKS = {5: 2, 6: 5, 7: 8, 8: 11, 9: 15, 10: 19}


def add_into(dst, src, rows):
    step = min(rows, 288)

    def body(part):
        dst[part, :] = dst[part, :] + src[part, :]

    if rows == step:
        dst[...] = dst[...] + src[...]
    else:
        row_loop(rows, step, body)


def backward_kernel(
    hid, slope, x_in, x_mid, w_in_b, w_out_b, d_top, d_hid_top, extra, total, images_all,
    unit, r0, r1, r2, r3, r4, b_slope, b_hid, b_in, b_out, d_pre, d_x, n, x_buf, d_n,
    load_sem, x_sem, send_sem, recv_sem, local_sem, extra_send, extra_recv, extra_local, *, tokens, image, chunks,
):
    me = lax.axis_index("data")
    core, x_bit, y_bit = me % 2, (me // 2) % 2, (me // 4) % 2
    z_low, z_high = (me // 8) % 2, me // 16
    bits = ((x_bit, z_low, y_bit, z_high), (y_bit, z_low, x_bit, z_high))
    flips = {1: core, 2: x_bit, 4: y_bit, 8: z_low, 16: z_high}

    def peer(mask):
        return (me + mask * (1 - 2 * flips[mask]),)

    def rows_at(start, size):
        return pl.ds(pl.multiple_of(start, 16), size)

    def remote(src, dst, send, recv, mask):
        return pltpu.make_async_remote_copy(
            src_ref=src, dst_ref=dst, send_sem=send, recv_sem=recv, device_id=peer(mask), device_id_type=MESH
        )

    def base(stream, color, level):
        start = stream * STREAM + core * HALF + color * COLOR
        for step in range(level):
            start = start + bits[color][step] * SIZES[step]
        return start

    def lanes_at(bit):
        return pl.ds(pl.multiple_of(bit * 128, 128), 128)

    def piece_of(stream, color, pair):
        return total.at[pair, rows_at(base(stream, color, 3), SIZES[2]), lanes_at(z_high)]

    def copy_of(stage, stream, color, pair, slot):
        bit = bits[color]
        if stage == 0:
            src = unit.at[slot, rows_at(stream * STREAM + (1 - core) * HALF, HALF)]
            dst, mask = r0.at[slot, stream], 1
        elif stage == 1:
            src = r0.at[slot, stream, rows_at(color * COLOR + (1 - bit[0]) * SIZES[0], SIZES[0])]
            dst, mask = r1.at[pair % 3, stream, color], MASKS[color][0]
        elif stage <= 3:
            size = SIZES[stage - 1]
            src = (r1, r2)[stage - 2].at[(pair % 3, slot)[stage - 2], stream, color, rows_at((1 - bit[stage - 1]) * size, size)]
            dst, mask = (r2, r3)[stage - 2].at[slot, stream, color], MASKS[color][stage - 1]
        elif stage == 4:
            src = r3.at[slot, stream, color, :, lanes_at(1 - z_high)]
            dst, mask = r4.at[slot, stream, color], 16
        elif stage == 5:
            src = dst = piece_of(stream, color, pair)
            mask = 16
        elif stage <= 8:
            level = 9 - stage
            src = dst = total.at[pair, rows_at(base(stream, color, level), SIZES[level - 1])]
            mask = MASKS[color][level - 1]
        else:
            src = dst = total.at[pair, rows_at(base(stream, color, 0), COLOR)]
            mask = 1
        at = (stage, color, slot, stream)
        return remote(src, dst, send_sem.at[at], recv_sem.at[at], mask)

    def own_copy(stream, color, pair, slot):
        return pltpu.make_async_copy(
            r4.at[slot, stream, color], piece_of(stream, color, pair), local_sem.at[color, slot, stream]
        )

    def reduce_stage(stage, stream, pair):
        slot = pair % 2
        if stage == 0:
            copy_of(0, stream, 0, pair, slot).start()
            return
        if stage == 1:
            copy_of(0, stream, 0, pair, slot).wait()
            add_into(r0.at[slot, stream], unit.at[slot, rows_at(stream * STREAM + core * HALF, HALF)], HALF)
        for color in range(2):
            bit = bits[color]
            if 2 <= stage <= 5:
                copy_of(stage - 1, stream, color, pair, slot).wait()
            if stage == 2:
                kept = r0.at[slot, stream, rows_at(color * COLOR + bit[0] * SIZES[0], SIZES[0])]
                add_into(r1.at[pair % 3, stream, color], kept, SIZES[0])
            elif stage in (3, 4):
                size = SIZES[stage - 2]
                kept = (r1, r2)[stage - 3].at[(pair % 3, slot)[stage - 3], stream, color, rows_at(bit[stage - 2] * size, size)]
                add_into((r2, r3)[stage - 3].at[slot, stream, color], kept, size)
            elif stage == 5:
                kept = r3.at[slot, stream, color, :, lanes_at(z_high)]
                add_into(r4.at[slot, stream, color], kept, SIZES[2])
        for color in range(2):
            if stage <= 4:
                copy_of(stage, stream, color, pair, slot).start()
            elif stage == 5:
                own_copy(stream, color, pair, slot).start()
            else:
                own_copy(stream, color, pair, slot).wait()

    def gather_step(step, stream, pair):
        slot = pair % 2
        for color in range(2):
            if step > 0:
                copy_of(4 + step, stream, color, pair, slot).wait()
            if step < len(GATHER) - 1:
                copy_of(5 + step, stream, color, pair, slot).start()

    def exchange(tick, first=False):
        def at(offset, stream, action):
            ahead = tick - READY[stream] - offset

            @pl.when((ahead >= 0) & (ahead < 3 * PAIRS) & (ahead % 3 == 0))
            def _():
                action(ahead // 3)

        for stage in reversed(range(2 if first else len(REDUCE))):
            for stream in range(2):
                at(REDUCE[stage], stream, functools.partial(reduce_stage, stage, stream))
        for step in reversed(range(0 if first else len(GATHER))):
            for stream in range(2):
                at(GATHER[step], stream, functools.partial(gather_step, step, stream))

    def extra_rows(level):
        start, size = core * 16, 16
        for step in range(level):
            size = size // 2
            start = start + bits[0][step] * size
        return images_all.at[:, pl.ds(pl.multiple_of(start * 8, 8), size * 8)]

    def extra_copy(stage):
        spot = extra_rows(9 - stage)
        mask = 1 if stage == 9 else MASKS[0][8 - stage]
        src = extra if stage == 5 else spot
        return remote(src, spot, extra_send.at[stage - 5], extra_recv.at[stage - 5], mask)

    def exchange_extra(stage):
        if stage > 5:
            extra_copy(stage - 1).wait()
        if stage == 6:
            pltpu.make_async_copy(extra, extra_rows(4), extra_local).wait()
        if stage == 5:
            pltpu.make_async_copy(extra, extra_rows(4), extra_local).start()
        if stage <= 9:
            extra_copy(stage).start()

    def run_extra(tick, ticks):
        for stage, when in EXTRA_TICKS.items():
            if when in ticks:
                @pl.when(tick == when)
                def _():
                    exchange_extra(stage)

    def load_chunk(tick, top=False):
        layer, chunk, slot = 3 - tick // chunks, tick % chunks, tick % 2
        cols = pl.ds(pl.multiple_of(chunk * CHUNK, CHUNK), CHUNK)
        arrays = [(slope.at[layer, chunk], b_slope), (w_in_b.at[layer, :, cols], b_in)]
        if not top:
            arrays += [(hid.at[layer, chunk], b_hid), (w_out_b.at[layer, cols, :], b_out)]
        return [pltpu.make_async_copy(src, dst.at[slot], load_sem.at[slot, i]) for i, (src, dst) in enumerate(arrays)]

    def load_x(layer):
        return pltpu.make_async_copy(x_mid.at[layer - 1], x_buf.at[layer % 2], x_sem.at[layer % 2])

    load_bottom = pltpu.make_async_copy(x_in, x_buf.at[0], x_sem.at[0])

    for load in load_chunk(0, True):
        load.start()
    load_x(3).start()
    load_x(2).start()

    barrier = pltpu.get_barrier_semaphore()
    for mask in flips:
        pl.semaphore_signal(barrier, inc=1, device_id=peer(mask), device_id_type=MESH)

    def store_in(slot, block, value):
        value = value.astype(BF16)
        for half in range(CHUNK // LANES):
            rows = pl.ds(pl.multiple_of(block * 1536 + half * 768, 16), 768)
            unit[slot, rows, :] = value[:, span(half, LANES)]

    def store_out(slot, block, value):
        value = value.astype(BF16)
        for third in range(768 // LANES):
            rows = pl.ds(pl.multiple_of(block * 1536 + third * CHUNK, 16), CHUNK)
            unit[slot, rows, :] = value[:, span(third, LANES)]

    tile = 768

    def add_d_n(slot):
        for i in range(tokens // tile):
            rows = span(i, tile)
            d_n[rows, :] = dot_rhs_t(d_pre[rows, :], b_in[slot]) + d_n[rows, :]

    load_x(3).wait()

    def start_top(rows):
        n[rows, :] = norm_rows(x_buf[1, rows, :].astype(F32)).astype(BF16)
        d_n[rows, :] = jnp.zeros_like(d_n[rows, :])

    row_loop(tokens, ROWS, start_top)
    for i in range(tokens // image):
        d_x[span(i, image), :] = jnp.broadcast_to(d_top[span(i, 1), :], (image, d_top.shape[1])).astype(BF16)

    pl.semaphore_wait(barrier, len(flips))

    @pl.loop(0, chunks)
    def _(tick):
        slot = tick % 2
        for load in load_chunk(tick, True):
            load.wait()

        @pl.when(tick < chunks - 1)
        def _():
            for load in load_chunk(tick + 1, True):
                load.start()

        @pl.when(tick == chunks - 1)
        def _():
            for load in load_chunk(tick + 1):
                load.start()

        for i in range(tokens // image):
            rows = span(i, image)
            d_pre[rows, :] = (b_slope[slot, rows, :].astype(F32) * d_hid_top[tick, span(i, 1), :]).astype(BF16)
        store_in(0, tick, dot_lhs_t(n[...], d_pre[...]))
        add_d_n(slot)
        exchange(tick, True)
        run_extra(tick, range(chunks))

    @pl.loop(chunks, TICKS)
    def _(tick):
        layer, chunk, slot = 3 - tick // chunks, tick % chunks, tick % 2
        use = (tick // 3 - 1) % 2

        @pl.when(chunk == 0)
        def _():
            upper, lower = (layer + 1) % 2, layer % 2
            pltpu.make_async_copy(x_in, x_buf.at[lower], x_sem.at[lower]).wait()

            def step(rows):
                centered, inv_std = norm_stats(x_buf[upper, rows, :].astype(F32))
                x_hat = centered * inv_std
                grad = d_n[rows, :]
                mean_g = jnp.mean(grad, axis=-1, keepdims=True)
                mean_gx = jnp.mean(grad * x_hat, axis=-1, keepdims=True)
                d_x[rows, :] = (d_x[rows, :].astype(F32) + inv_std * (grad - mean_g - x_hat * mean_gx)).astype(BF16)
                n[rows, :] = norm_rows(x_buf[lower, rows, :].astype(F32)).astype(BF16)
                d_n[rows, :] = jnp.zeros_like(d_n[rows, :])

            row_loop(tokens, ROWS, step)

            @pl.when(layer == 2)
            def _():
                load_x(1).start()

            @pl.when(layer == 1)
            def _():
                load_bottom.start()

        for load in load_chunk(tick):
            load.wait()

        @pl.when(tick < TICKS - 1)
        def _():
            for load in load_chunk(tick + 1):
                load.start()

        for i in range(tokens // tile):
            rows = span(i, tile)
            d_pre[rows, :] = (dot_rhs_t(d_x[rows, :], b_out[slot]) * b_slope[slot, rows, :].astype(F32)).astype(BF16)
        store_out(use, 2 * (chunk % 3) + 1, dot_lhs_t(b_hid[slot], d_x[...]))
        store_in(use, 2 * (chunk % 3), dot_lhs_t(n[...], d_pre[...]))

        @pl.when(layer > 0)
        def _():
            add_d_n(slot)

        exchange(tick)
        run_extra(tick, range(chunks, TICKS))

    @pl.loop(TICKS, LAST_TICK)
    def _(tick):
        exchange(tick)


def backward(hid, slope, x_in, x_mid, w_in_b, w_out_b, d_top, d_hid_top, extra, image):
    layers, chunks, tokens, _ = hid.shape
    dim = x_in.shape[1]
    hbm = pl.BlockSpec(memory_space=pl.ANY)
    vmem = pl.BlockSpec(memory_space=pltpu.VMEM)
    act = pltpu.VMEM((tokens, dim), BF16)
    dma = pltpu.SemaphoreType.DMA
    return pl.pallas_call(
        functools.partial(backward_kernel, tokens=tokens, image=image, chunks=chunks),
        in_specs=[hbm] * 6 + [vmem] * 3,
        out_specs=[hbm, hbm],
        out_shape=[
            jax.ShapeDtypeStruct((PAIRS, 2 * STREAM, LANES), BF16),
            jax.ShapeDtypeStruct((GROUPS, 256, LANES), BF16),
        ],
        scratch_shapes=[
            pltpu.VMEM((2, 2 * STREAM, LANES), BF16),
            pltpu.VMEM((2, 2, HALF, LANES), BF16),
            *[pltpu.VMEM((slots, 2, 2, size, LANES), BF16) for slots, size in zip((3, 2, 2), SIZES)],
            pltpu.VMEM((2, 2, 2, SIZES[2], 128), BF16),
            pltpu.VMEM((2, tokens, CHUNK), BF16),
            pltpu.VMEM((2, tokens, CHUNK), BF16),
            pltpu.VMEM((2, dim, CHUNK), BF16),
            pltpu.VMEM((2, CHUNK, dim), BF16),
            pltpu.VMEM((tokens, CHUNK), BF16),
            act,
            act,
            pltpu.VMEM((2, tokens, dim), BF16),
            pltpu.VMEM((tokens, dim), F32),
            dma((2, 4)),
            dma((2,)),
            dma((10, 2, 2, 2)),
            dma((10, 2, 2, 2)),
            dma((2, 2, 2)),
            dma((5,)),
            dma((5,)),
            dma,
        ],
        compiler_params=pltpu.CompilerParams(vmem_limit_bytes=VMEM_LIMIT, collective_id=0, has_side_effects=True),
        name="backward",
    )(hid, slope, x_in, x_mid, w_in_b, w_out_b, d_top, d_hid_top, extra)


SLOTS = 3


def update_kernel(
    rates, x_hbm, w_in, m_in, w_out, m_out, grads, images_all, w_head, m_head,
    new_w_in, new_m_in, new_w_out, new_m_out, new_w_head, new_m_head, next_logits,
    b_w_in, b_m_in, b_w_out, b_m_out, b_g_in, b_g_out, rows_all, x, n, acc, pre, hid, w_in_b, w_out_b,
    load_sem, store_sem, x_sem, rows_sem, *, tokens, image, tile, chunks, layers,
):
    rate, coef = rates[0], rates[1]
    steps = layers * chunks

    def place(step):
        layer, chunk = step // chunks, step % chunks
        cols = pl.ds(pl.multiple_of(chunk * CHUNK, CHUNK), CHUNK)
        return layer, chunk, cols, step % SLOTS

    def loads(step):
        layer, chunk, cols, slot = place(step)
        top = layer // (layers - 1)
        lower = (1 + 2 * (layers - 2 - layer) + chunk // 3) * 6 + 2 * (chunk % 3)
        block = top * chunk + (1 - top) * lower
        arrays = (
            (w_in.at[layer, :, cols], b_w_in),
            (m_in.at[layer, :, cols], b_m_in),
            (w_out.at[layer, cols, :], b_w_out),
            (m_out.at[layer, cols, :], b_m_out),
            (grads.at[block], b_g_in),
            (grads.at[block + 1 - top], b_g_out),
        )
        return [pltpu.make_async_copy(src, dst.at[slot], load_sem.at[slot, i]) for i, (src, dst) in enumerate(arrays)]

    def stores(step):
        layer, chunk, cols, slot = place(step)
        arrays = (
            (b_w_in, new_w_in.at[layer, :, cols]),
            (b_m_in, new_m_in.at[layer, :, cols]),
            (b_w_out, new_w_out.at[layer, cols, :]),
            (b_m_out, new_m_out.at[layer, cols, :]),
        )
        return [pltpu.make_async_copy(src.at[slot], dst, store_sem.at[slot, i]) for i, (src, dst) in enumerate(arrays)]

    load_x = pltpu.make_async_copy(x_hbm, x, x_sem)
    load_rows = pltpu.make_async_copy(images_all, rows_all, rows_sem)
    load_x.start()
    for ahead in range(SLOTS - 1):
        for load in loads(ahead):
            load.start()
    load_rows.start()
    load_x.wait()

    def start(rows):
        n[rows, :] = norm_rows(x[rows, :].astype(F32)).astype(BF16)
        acc[rows, :] = jnp.zeros_like(acc[rows, :])

    row_loop(tokens, 128, start)

    load_rows.wait()
    classes = w_head.shape[0]
    for group in range(0, classes, LANES):
        size = min(LANES, classes - group)
        for part in range(3):
            at = (slice(group, group + size), span(part, LANES))
            grad = dot_lhs_t(rows_all[18 + group // LANES], rows_all[15 + part])[:size]
            moment = coef * m_head[at] + grad
            new_m_head[at] = moment
            new_w_head[at] = w_head[at] - rate * moment

    @pl.loop(0, steps)
    def _(step):
        layer, chunk, _, slot = place(step)
        for load in loads(step):
            load.wait()

        for half in range(CHUNK // LANES):
            cols = span(half, LANES)
            moment = coef * b_m_in[slot, :, cols] + b_g_in[slot, span(half, b_w_in.shape[1]), :].astype(F32)
            weight = b_w_in[slot, :, cols] - rate * moment
            b_m_in[slot, :, cols] = moment
            b_w_in[slot, :, cols] = weight
            w_in_b[:, cols] = weight.astype(BF16)

        def update_out(grad_of):
            for third in range(768 // LANES):
                cols = span(third, LANES)
                moment = coef * b_m_out[slot, :, cols] + grad_of(third)
                weight = b_w_out[slot, :, cols] - rate * moment
                b_m_out[slot, :, cols] = moment
                b_w_out[slot, :, cols] = weight
                w_out_b[:, cols] = weight.astype(BF16)

        @pl.when(layer < layers - 1)
        def _():
            update_out(lambda third: b_g_out[slot, span(third, CHUNK), :].astype(F32))

        @pl.when(layer == layers - 1)
        def _():
            def top_grad(third):
                parts = [dot_lhs_t(rows_all[2 * chunk + half], rows_all[12 + third]) for half in range(2)]
                return jnp.concatenate(parts, axis=0)

            update_out(top_grad)

        for store in stores(step):
            store.start()

        @pl.when(step >= 1)
        def _():
            for store in stores(step - 1):
                store.wait()

        @pl.when(step + SLOTS - 1 < steps)
        def _():
            for load in loads(step + SLOTS - 1):
                load.start()

        def first(i):
            pre[i % 2] = dot(n[span(i, tile), :], w_in_b[...])

        def act(i):
            for j in range(tile // ACT_ROWS):
                rows = span(j, ACT_ROWS)
                hid[i % 2, rows, :] = gelu_parts(pre[i % 2, rows, :])[-1].astype(BF16)

        def second(i):
            rows = span(i, tile)
            acc[rows, :] = dot(hid[i % 2], w_out_b[...]) + acc[rows, :]

        count = tokens // tile
        for i in range(count + 2):
            if i < count:
                first(i)
            if 0 <= i - 1 < count:
                act(i - 1)
            if i >= 2:
                second(i - 2)

        @pl.when(chunk == chunks - 1)
        def _():
            def finish(rows):
                value = (x[rows, :].astype(F32) + acc[rows, :]).astype(BF16)
                x[rows, :] = value
                n[rows, :] = norm_rows(value.astype(F32)).astype(BF16)
                acc[rows, :] = jnp.zeros_like(acc[rows, :])

            row_loop(tokens, 128, finish)

    pooled = (image_sums(x[...], image) / image).astype(BF16)
    next_logits[...] = dot_rhs_t(pooled, new_w_head[...].astype(BF16))
    for store in stores(steps - 1):
        store.wait()


def update_and_next(rates, x, w_in, m_in, w_out, m_out, total, images_all, w_head, m_head, image=576):
    tokens, dim = x.shape
    layers, _, hidden = w_in.shape
    chunks = hidden // CHUNK
    tile = 384
    hbm = pl.BlockSpec(memory_space=pl.ANY)
    vmem = pl.BlockSpec(memory_space=pltpu.VMEM)
    dma = pltpu.SemaphoreType.DMA
    return pl.pallas_call(
        functools.partial(update_kernel, tokens=tokens, image=image, tile=tile, chunks=chunks, layers=layers),
        in_specs=[pl.BlockSpec(memory_space=pltpu.SMEM)] + [hbm] * 7 + [vmem] * 2,
        out_specs=[hbm] * 4 + [vmem] * 3,
        out_shape=[
            jax.ShapeDtypeStruct(w_in.shape, F32),
            jax.ShapeDtypeStruct(w_in.shape, F32),
            jax.ShapeDtypeStruct(w_out.shape, F32),
            jax.ShapeDtypeStruct(w_out.shape, F32),
            jax.ShapeDtypeStruct(w_head.shape, F32),
            jax.ShapeDtypeStruct(w_head.shape, F32),
            jax.ShapeDtypeStruct((8, w_head.shape[0]), F32),
        ],
        scratch_shapes=[
            pltpu.VMEM((SLOTS, dim, CHUNK), F32),
            pltpu.VMEM((SLOTS, dim, CHUNK), F32),
            pltpu.VMEM((SLOTS, CHUNK, dim), F32),
            pltpu.VMEM((SLOTS, CHUNK, dim), F32),
            pltpu.VMEM((SLOTS, 1536, LANES), BF16),
            pltpu.VMEM((SLOTS, 1536, LANES), BF16),
            pltpu.VMEM((GROUPS, 256, LANES), BF16),
            pltpu.VMEM((tokens, dim), BF16),
            pltpu.VMEM((tokens, dim), BF16),
            pltpu.VMEM((tokens, dim), F32),
            pltpu.VMEM((2, tile, CHUNK), F32),
            pltpu.VMEM((2, tile, CHUNK), BF16),
            pltpu.VMEM((dim, CHUNK), BF16),
            pltpu.VMEM((CHUNK, dim), BF16),
            dma((SLOTS, 6)),
            dma((SLOTS, 4)),
            dma,
            dma,
        ],
        compiler_params=pltpu.CompilerParams(vmem_limit_bytes=VMEM_LIMIT),
        name="update_next",
    )(rates, x, w_in, m_in, w_out, m_out, total.reshape(PAIRS * 6, 1536, LANES), images_all, w_head, m_head)


def solution(mesh):
    group_size = mesh.shape["data"]

    def local_step(x_step, labels, x_next, w_in, w_out, w_head, mom_in, mom_out, mom_head, learn_rate, mom_coef):
        micro, per_micro, image, dim = x_step.shape
        images = micro * per_micro
        layers, _, hidden = w_in.shape
        classes = w_head.shape[1]
        chunks = hidden // CHUNK
        examples = images * group_size
        w_head_b = w_head.astype(BF16)

        x_in = x_step.reshape(images * image, dim)
        hid, slope, w_in_b, w_out_b, x_mid, hid_sum, top_sum = forward(x_in, w_in, w_out, image)

        pooled = (top_sum[:images] / image).astype(BF16)
        soft_prob = jax.nn.softmax(dot(pooled, w_head_b), axis=-1)
        onehot = (labels.reshape(images, 1) == jnp.arange(classes)[None, :]).astype(F32)
        d_logits = ((soft_prob - onehot) / examples).astype(BF16)
        d_top = (dot_rhs_t(d_logits, w_head_b) / image).astype(BF16)
        d_hid_top = dot_rhs_t(d_top, w_out_b[layers - 1])
        d_hid_top = jnp.pad(d_hid_top, ((0, 8 - images), (0, 0))).reshape(8, chunks, CHUNK).transpose(1, 0, 2)

        hid_sum = hid_sum[:, :images].transpose(1, 0, 2).reshape(images, hidden)
        hid_high = lax.reduce_precision(hid_sum, 8, 7)
        hid_low = (hid_sum - hid_high).astype(BF16)
        wide = lambda a, b: jnp.concatenate([a, b]).reshape(2 * images, -1, LANES).transpose(1, 0, 2)
        logit_pad = jnp.pad(d_logits, ((0, 0), (0, 1024 - classes)))
        extra = jnp.concatenate([
            wide(hid_high.astype(BF16), hid_low),
            wide(d_top, d_top),
            wide(pooled, jnp.zeros_like(pooled)),
            wide(logit_pad, jnp.zeros_like(logit_pad)),
        ])

        total, images_all = backward(
            hid, slope, x_in, x_mid, w_in_b, w_out_b,
            jnp.pad(d_top.astype(F32), ((0, 8 - images), (0, 0))), d_hid_top, extra, image,
        )

        rates = jnp.stack([learn_rate, mom_coef])
        x_last = x_next.reshape(-1, dim)
        new_w_in, new_mom_in, new_w_out, new_mom_out, new_w_head, new_mom_head, logits_next = update_and_next(
            rates, x_last, w_in, mom_in, w_out, mom_out, total, images_all, w_head.T, mom_head.T, image
        )
        logits_next, new_w_head, new_mom_head = logits_next[: x_next.shape[0]], new_w_head.T, new_mom_head.T
        return (logits_next, new_w_in, new_w_out, new_w_head, new_mom_in, new_mom_out, new_mom_head)

    return jax.shard_map(
        local_step,
        mesh=mesh,
        in_specs=(P(None, "data", None, None), P(None, "data"), P("data", None, None), P(), P(), P(), P(), P(), P(), P(), P()),
        out_specs=(P("data", None), P(), P(), P(), P(), P(), P()),
        check_vma=False,
    )
```

```python
import functools
import math

import jax
import jax.numpy as jnp
from jax import lax
from jax.experimental import pallas as pl
from jax.experimental.pallas import tpu as pltpu
from jax.sharding import PartitionSpec as P

BF16 = jnp.bfloat16
F32 = jnp.float32
LN_EPS = 1e-6
C0 = math.sqrt(2.0 / math.pi)
C1 = 0.044715
CHUNK = 512
ROWS = 256
LANES = 256
FWD_TILE = 768
ACT_ROWS = 64
LN_ROWS = 96
MESH = pl.DeviceIdType.MESH
VMEM_LIMIT = 63 * 1024 * 1024


def norm_stats(x_f32):
    row_mean = jnp.mean(x_f32, axis=-1, keepdims=True)
    centered = x_f32 - row_mean
    inv_std = lax.rsqrt(jnp.mean(centered * centered, axis=-1, keepdims=True) + LN_EPS)
    return centered, inv_std


def norm_rows(x_f32):
    centered, inv_std = norm_stats(x_f32)
    return centered * inv_std


def gelu_parts(pre):
    squared = pre * pre
    gate = 0.5 + 0.5 * jnp.tanh(pre * (C0 + (C0 * C1) * squared))
    return squared, gate, pre * gate


def span(index, size):
    return slice(index * size, index * size + size)


def row_loop(total, step, body):
    @pl.loop(0, total // step)
    def _(index):
        body(pl.ds(pl.multiple_of(index * step, step), step))


def dot(a, b):
    return jnp.dot(a, b, preferred_element_type=F32)


def dot_rhs_t(a, b):
    return lax.dot_general(a, b, (((1,), (1,)), ((), ())), preferred_element_type=F32)


def dot_lhs_t(a, b):
    return lax.dot_general(a, b, (((0,), (0,)), ((), ())), preferred_element_type=F32)


def image_sums(x, image):
    rows = lax.broadcasted_iota(jnp.int32, (8, x.shape[0]), 0)
    cols = lax.broadcasted_iota(jnp.int32, (8, x.shape[0]), 1)
    inside = (cols >= rows * image) & (cols < (rows + 1) * image)
    return dot(inside.astype(F32).astype(BF16), x)


def forward_kernel(
    x_hbm, w_in, w_out, hid, slope, w_in_b, w_out_b, x_out, hid_sum, top_sum,
    x, n, acc, pre, sem, *, tokens, image, tile, layers, chunks,
):
    layer, chunk = pl.program_id(0), pl.program_id(1)

    @pl.when((layer == 0) & (chunk == 0))
    def _():
        load = pltpu.make_async_copy(x_hbm, x, sem)
        load.start()
        load.wait()

    w_in_b[...] = w_in[...].astype(BF16)
    w_out_b[...] = w_out[...].astype(BF16)

    def first(i):
        pre[i % 2] = dot(n[span(i, tile), :], w_in_b[...])

    def act(i):
        for j in range(tile // ACT_ROWS):
            rows = span(i * tile // ACT_ROWS + j, ACT_ROWS)
            squared, gate, value = gelu_parts(pre[i % 2, span(j, ACT_ROWS), :])
            hid[rows, :] = value.astype(BF16)
            slope[rows, :] = (gate + (value * (2 * C0 + (6 * C0 * C1) * squared)) * (1.0 - gate)).astype(BF16)

    def second(i, begin):
        rows = span(i, tile)
        part = dot(hid[rows, :], w_out_b[...])
        acc[rows, :] = part if begin else part + acc[rows, :]

    def begin_rows(i):
        for j in range(tile // LN_ROWS):
            rows = span(i * tile // LN_ROWS + j, LN_ROWS)
            n[rows, :] = norm_rows(x[rows, :].astype(F32)).astype(BF16)

    def end_rows(i):
        for j in range(tile // LN_ROWS):
            rows = span(i * tile // LN_ROWS + j, LN_ROWS)
            value = (x[rows, :].astype(F32) + acc[rows, :]).astype(BF16)
            x[rows, :] = value
            x_out[rows, :] = value

    def run(begin, end):
        steps = [begin_rows] * begin + [first, act, functools.partial(second, begin=begin)] + [end_rows] * end
        count = tokens // tile
        for i in range(count + len(steps) - 1):
            for lag, step in enumerate(steps):
                if 0 <= i - lag < count:
                    step(i - lag)

    @pl.when(chunk == 0)
    def _():
        run(True, False)

    @pl.when((chunk > 0) & (chunk < chunks - 1))
    def _():
        run(False, False)

    @pl.when(chunk == chunks - 1)
    def _():
        run(False, True)

    @pl.when(layer == layers - 1)
    def _():
        hid_sum[...] = image_sums(hid[...], image)

        @pl.when(chunk == chunks - 1)
        def _():
            top_sum[...] = image_sums(x[...], image)


def forward(x, w_in, w_out, image=576):
    tokens, dim = x.shape
    layers, _, hidden = w_in.shape
    chunks = hidden // CHUNK
    top = layers - 1
    one = pl.squeezed
    in_spec = pl.BlockSpec((one, dim, CHUNK), lambda l, f: (l, 0, f))
    out_spec = pl.BlockSpec((one, CHUNK, dim), lambda l, f: (l, f, 0))
    act = jax.ShapeDtypeStruct((layers, chunks, tokens, CHUNK), BF16)
    return pl.pallas_call(
        functools.partial(forward_kernel, tokens=tokens, image=image, tile=FWD_TILE, layers=layers, chunks=chunks),
        grid=(layers, chunks),
        in_specs=[pl.BlockSpec(memory_space=pl.ANY), in_spec, out_spec],
        out_specs=[
            pl.BlockSpec((one, one, tokens, CHUNK), lambda l, f: (l, jnp.where(l == top, 0, f), 0, 0)),
            pl.BlockSpec((one, one, tokens, CHUNK), lambda l, f: (l, f, 0, 0)),
            in_spec,
            out_spec,
            pl.BlockSpec((one, tokens, dim), lambda l, f: (l, 0, 0)),
            pl.BlockSpec((one, 8, CHUNK), lambda l, f: (jnp.where(l == top, f, 0), 0, 0)),
            pl.BlockSpec((8, dim), lambda l, f: (0, 0)),
        ],
        out_shape=[
            act,
            act,
            jax.ShapeDtypeStruct(w_in.shape, BF16),
            jax.ShapeDtypeStruct(w_out.shape, BF16),
            jax.ShapeDtypeStruct((layers, tokens, dim), BF16),
            jax.ShapeDtypeStruct((chunks, 8, CHUNK), F32),
            jax.ShapeDtypeStruct((8, dim), F32),
        ],
        scratch_shapes=[
            pltpu.VMEM((tokens, dim), BF16),
            pltpu.VMEM((tokens, dim), BF16),
            pltpu.VMEM((tokens, dim), F32),
            pltpu.VMEM((2, FWD_TILE, CHUNK), F32),
            pltpu.SemaphoreType.DMA,
        ],
        compiler_params=pltpu.CompilerParams(vmem_limit_bytes=VMEM_LIMIT),
        name="forward",
    )(x, w_in, w_out)


PAIRS = 7
STREAM = 4608
HALF = 2304
COLOR = 1152
SIZES = (576, 288, 144)
MASKS = ((2, 8, 4, 16), (4, 8, 2, 16))
READY = (4, 5)
REDUCE = (0, 1, 3, 5, 6, 7, 8)
GATHER = (8, 9, 10, 12, 14, 15)
TICKS = 24
LAST_TICK = READY[1] + 3 * (PAIRS - 1) + GATHER[-1] + 1
GROUPS = 11
EXTRA_TICKS = {5: 2, 6: 5, 7: 8, 8: 11, 9: 15, 10: 19}


def add_into(dst, src, rows):
    step = min(rows, 288)

    def body(part):
        dst[part, :] = dst[part, :] + src[part, :]

    if rows == step:
        dst[...] = dst[...] + src[...]
    else:
        row_loop(rows, step, body)


def backward_kernel(
    hid, slope, x_in, x_mid, w_in_b, w_out_b, d_top, d_hid_top, extra, total, images_all,
    unit, r0, r1, r2, r3, r4, b_slope, b_hid, b_in, b_out, d_pre, d_x, n, x_buf, d_n,
    load_sem, x_sem, send_sem, recv_sem, local_sem, extra_send, extra_recv, extra_local, *, tokens, image, chunks,
):
    me = lax.axis_index("data")
    core, x_bit, y_bit = me % 2, (me // 2) % 2, (me // 4) % 2
    z_low, z_high = (me // 8) % 2, me // 16
    bits = ((x_bit, z_low, y_bit, z_high), (y_bit, z_low, x_bit, z_high))
    flips = {1: core, 2: x_bit, 4: y_bit, 8: z_low, 16: z_high}

    def peer(mask):
        return (me + mask * (1 - 2 * flips[mask]),)

    def rows_at(start, size):
        return pl.ds(pl.multiple_of(start, 16), size)

    def remote(src, dst, send, recv, mask):
        return pltpu.make_async_remote_copy(
            src_ref=src, dst_ref=dst, send_sem=send, recv_sem=recv, device_id=peer(mask), device_id_type=MESH
        )

    def base(stream, color, level):
        start = stream * STREAM + core * HALF + color * COLOR
        for step in range(level):
            start = start + bits[color][step] * SIZES[step]
        return start

    def lanes_at(bit):
        return pl.ds(pl.multiple_of(bit * 128, 128), 128)

    def piece_of(stream, color, pair):
        return total.at[pair, rows_at(base(stream, color, 3), SIZES[2]), lanes_at(z_high)]

    def copy_of(stage, stream, color, pair, slot):
        bit = bits[color]
        if stage == 0:
            src = unit.at[slot, rows_at(stream * STREAM + (1 - core) * HALF, HALF)]
            dst, mask = r0.at[slot, stream], 1
        elif stage == 1:
            src = r0.at[slot, stream, rows_at(color * COLOR + (1 - bit[0]) * SIZES[0], SIZES[0])]
            dst, mask = r1.at[pair % 3, stream, color], MASKS[color][0]
        elif stage <= 3:
            size = SIZES[stage - 1]
            src = (r1, r2)[stage - 2].at[(pair % 3, slot)[stage - 2], stream, color, rows_at((1 - bit[stage - 1]) * size, size)]
            dst, mask = (r2, r3)[stage - 2].at[slot, stream, color], MASKS[color][stage - 1]
        elif stage == 4:
            src = r3.at[slot, stream, color, :, lanes_at(1 - z_high)]
            dst, mask = r4.at[slot, stream, color], 16
        elif stage == 5:
            src = dst = piece_of(stream, color, pair)
            mask = 16
        elif stage <= 8:
            level = 9 - stage
            src = dst = total.at[pair, rows_at(base(stream, color, level), SIZES[level - 1])]
            mask = MASKS[color][level - 1]
        else:
            src = dst = total.at[pair, rows_at(base(stream, color, 0), COLOR)]
            mask = 1
        at = (stage, color, slot, stream)
        return remote(src, dst, send_sem.at[at], recv_sem.at[at], mask)

    def own_copy(stream, color, pair, slot):
        return pltpu.make_async_copy(
            r4.at[slot, stream, color], piece_of(stream, color, pair), local_sem.at[color, slot, stream]
        )

    def reduce_stage(stage, stream, pair):
        slot = pair % 2
        if stage == 0:
            copy_of(0, stream, 0, pair, slot).start()
            return
        if stage == 1:
            copy_of(0, stream, 0, pair, slot).wait()
            add_into(r0.at[slot, stream], unit.at[slot, rows_at(stream * STREAM + core * HALF, HALF)], HALF)
        for color in range(2):
            bit = bits[color]
            if 2 <= stage <= 5:
                copy_of(stage - 1, stream, color, pair, slot).wait()
            if stage == 2:
                kept = r0.at[slot, stream, rows_at(color * COLOR + bit[0] * SIZES[0], SIZES[0])]
                add_into(r1.at[pair % 3, stream, color], kept, SIZES[0])
            elif stage in (3, 4):
                size = SIZES[stage - 2]
                kept = (r1, r2)[stage - 3].at[(pair % 3, slot)[stage - 3], stream, color, rows_at(bit[stage - 2] * size, size)]
                add_into((r2, r3)[stage - 3].at[slot, stream, color], kept, size)
            elif stage == 5:
                kept = r3.at[slot, stream, color, :, lanes_at(z_high)]
                add_into(r4.at[slot, stream, color], kept, SIZES[2])
        for color in range(2):
            if stage <= 4:
                copy_of(stage, stream, color, pair, slot).start()
            elif stage == 5:
                own_copy(stream, color, pair, slot).start()
            else:
                own_copy(stream, color, pair, slot).wait()

    def gather_step(step, stream, pair):
        slot = pair % 2
        for color in range(2):
            if step > 0:
                copy_of(4 + step, stream, color, pair, slot).wait()
            if step < len(GATHER) - 1:
                copy_of(5 + step, stream, color, pair, slot).start()

    def exchange(tick, first=False):
        def at(offset, stream, action):
            ahead = tick - READY[stream] - offset

            @pl.when((ahead >= 0) & (ahead < 3 * PAIRS) & (ahead % 3 == 0))
            def _():
                action(ahead // 3)

        for stage in reversed(range(2 if first else len(REDUCE))):
            for stream in range(2):
                at(REDUCE[stage], stream, functools.partial(reduce_stage, stage, stream))
        for step in reversed(range(0 if first else len(GATHER))):
            for stream in range(2):
                at(GATHER[step], stream, functools.partial(gather_step, step, stream))

    def extra_rows(color, level):
        start, size = core * 16, 16
        for step in range(level):
            size = size // 2
            start = start + bits[color][step] * size
        return images_all.at[color, :, pl.ds(pl.multiple_of(start * 8, 8), size * 8)]

    def extra_copy(stage, color):
        spot = extra_rows(color, 9 - stage)
        mask = 1 if stage == 9 else MASKS[color][8 - stage]
        src = extra.at[color] if stage == 5 else spot
        at = (stage - 5, color)
        return remote(src, spot, extra_send.at[at], extra_recv.at[at], mask)

    def extra_own(color):
        return pltpu.make_async_copy(extra.at[color], extra_rows(color, 4), extra_local.at[color])

    def exchange_extra(stage):
        for color in range(2):
            if stage > 5:
                extra_copy(stage - 1, color).wait()
            if stage == 6:
                extra_own(color).wait()
            if stage == 5:
                extra_own(color).start()
            if stage <= 9:
                extra_copy(stage, color).start()

    def run_extra(tick, ticks):
        for stage, when in EXTRA_TICKS.items():
            if when in ticks:
                @pl.when(tick == when)
                def _():
                    exchange_extra(stage)

    def load_chunk(tick, top=False):
        layer, chunk, slot = 3 - tick // chunks, tick % chunks, tick % 2
        cols = pl.ds(pl.multiple_of(chunk * CHUNK, CHUNK), CHUNK)
        arrays = [(slope.at[layer, chunk], b_slope), (w_in_b.at[layer, :, cols], b_in)]
        if not top:
            arrays += [(hid.at[layer, chunk], b_hid), (w_out_b.at[layer, cols, :], b_out)]
        return [pltpu.make_async_copy(src, dst.at[slot], load_sem.at[slot, i]) for i, (src, dst) in enumerate(arrays)]

    def load_x(layer):
        return pltpu.make_async_copy(x_mid.at[layer - 1], x_buf.at[layer % 2], x_sem.at[layer % 2])

    load_bottom = pltpu.make_async_copy(x_in, x_buf.at[0], x_sem.at[0])

    for load in load_chunk(0, True):
        load.start()
    load_x(3).start()
    load_x(2).start()

    barrier = pltpu.get_barrier_semaphore()
    for mask in flips:
        pl.semaphore_signal(barrier, inc=1, device_id=peer(mask), device_id_type=MESH)

    def store_in(slot, block, value):
        value = value.astype(BF16)
        for half in range(CHUNK // LANES):
            rows = pl.ds(pl.multiple_of(block * 1536 + half * 768, 16), 768)
            unit[slot, rows, :] = value[:, span(half, LANES)]

    def store_out(slot, block, value):
        value = value.astype(BF16)
        for third in range(768 // LANES):
            rows = pl.ds(pl.multiple_of(block * 1536 + third * CHUNK, 16), CHUNK)
            unit[slot, rows, :] = value[:, span(third, LANES)]

    tile = 768

    def add_d_n(slot):
        for i in range(tokens // tile):
            rows = span(i, tile)
            d_n[rows, :] = dot_rhs_t(d_pre[rows, :], b_in[slot]) + d_n[rows, :]

    load_x(3).wait()

    def start_top(rows):
        n[rows, :] = norm_rows(x_buf[1, rows, :].astype(F32)).astype(BF16)
        d_n[rows, :] = jnp.zeros_like(d_n[rows, :])

    row_loop(tokens, ROWS, start_top)
    for i in range(tokens // image):
        d_x[span(i, image), :] = jnp.broadcast_to(d_top[span(i, 1), :], (image, d_top.shape[1])).astype(BF16)

    pl.semaphore_wait(barrier, len(flips))

    @pl.loop(0, chunks)
    def _(tick):
        slot = tick % 2
        for load in load_chunk(tick, True):
            load.wait()

        @pl.when(tick < chunks - 1)
        def _():
            for load in load_chunk(tick + 1, True):
                load.start()

        @pl.when(tick == chunks - 1)
        def _():
            for load in load_chunk(tick + 1):
                load.start()

        for i in range(tokens // image):
            rows = span(i, image)
            d_pre[rows, :] = (b_slope[slot, rows, :].astype(F32) * d_hid_top[tick, span(i, 1), :]).astype(BF16)
        store_in(0, tick, dot_lhs_t(n[...], d_pre[...]))
        add_d_n(slot)
        exchange(tick, True)
        run_extra(tick, range(chunks))

    @pl.loop(chunks, TICKS)
    def _(tick):
        layer, chunk, slot = 3 - tick // chunks, tick % chunks, tick % 2
        use = (tick // 3 - 1) % 2

        @pl.when(chunk == 0)
        def _():
            upper, lower = (layer + 1) % 2, layer % 2
            pltpu.make_async_copy(x_in, x_buf.at[lower], x_sem.at[lower]).wait()

            def step(rows):
                centered, inv_std = norm_stats(x_buf[upper, rows, :].astype(F32))
                x_hat = centered * inv_std
                grad = d_n[rows, :]
                mean_g = jnp.mean(grad, axis=-1, keepdims=True)
                mean_gx = jnp.mean(grad * x_hat, axis=-1, keepdims=True)
                d_x[rows, :] = (d_x[rows, :].astype(F32) + inv_std * (grad - mean_g - x_hat * mean_gx)).astype(BF16)
                n[rows, :] = norm_rows(x_buf[lower, rows, :].astype(F32)).astype(BF16)
                d_n[rows, :] = jnp.zeros_like(d_n[rows, :])

            row_loop(tokens, ROWS, step)

            @pl.when(layer == 2)
            def _():
                load_x(1).start()

            @pl.when(layer == 1)
            def _():
                load_bottom.start()

        for load in load_chunk(tick):
            load.wait()

        @pl.when(tick < TICKS - 1)
        def _():
            for load in load_chunk(tick + 1):
                load.start()

        for i in range(tokens // tile):
            rows = span(i, tile)
            d_pre[rows, :] = (dot_rhs_t(d_x[rows, :], b_out[slot]) * b_slope[slot, rows, :].astype(F32)).astype(BF16)
        store_out(use, 2 * (chunk % 3) + 1, dot_lhs_t(b_hid[slot], d_x[...]))
        store_in(use, 2 * (chunk % 3), dot_lhs_t(n[...], d_pre[...]))

        @pl.when(layer > 0)
        def _():
            add_d_n(slot)

        exchange(tick)
        run_extra(tick, range(chunks, TICKS))

    @pl.loop(TICKS, LAST_TICK)
    def _(tick):
        exchange(tick)


def backward(hid, slope, x_in, x_mid, w_in_b, w_out_b, d_top, d_hid_top, extra, image):
    layers, chunks, tokens, _ = hid.shape
    dim = x_in.shape[1]
    hbm = pl.BlockSpec(memory_space=pl.ANY)
    vmem = pl.BlockSpec(memory_space=pltpu.VMEM)
    act = pltpu.VMEM((tokens, dim), BF16)
    dma = pltpu.SemaphoreType.DMA
    return pl.pallas_call(
        functools.partial(backward_kernel, tokens=tokens, image=image, chunks=chunks),
        in_specs=[hbm] * 6 + [vmem] * 3,
        out_specs=[hbm, hbm],
        out_shape=[
            jax.ShapeDtypeStruct((PAIRS, 2 * STREAM, LANES), BF16),
            jax.ShapeDtypeStruct((2, GROUPS, 256, LANES), BF16),
        ],
        scratch_shapes=[
            pltpu.VMEM((2, 2 * STREAM, LANES), BF16),
            pltpu.VMEM((2, 2, HALF, LANES), BF16),
            *[pltpu.VMEM((slots, 2, 2, size, LANES), BF16) for slots, size in zip((3, 2, 2), SIZES)],
            pltpu.VMEM((2, 2, 2, SIZES[2], 128), BF16),
            pltpu.VMEM((2, tokens, CHUNK), BF16),
            pltpu.VMEM((2, tokens, CHUNK), BF16),
            pltpu.VMEM((2, dim, CHUNK), BF16),
            pltpu.VMEM((2, CHUNK, dim), BF16),
            pltpu.VMEM((tokens, CHUNK), BF16),
            act,
            act,
            pltpu.VMEM((2, tokens, dim), BF16),
            pltpu.VMEM((tokens, dim), F32),
            dma((2, 4)),
            dma((2,)),
            dma((10, 2, 2, 2)),
            dma((10, 2, 2, 2)),
            dma((2, 2, 2)),
            dma((5, 2)),
            dma((5, 2)),
            dma((2,)),
        ],
        compiler_params=pltpu.CompilerParams(vmem_limit_bytes=VMEM_LIMIT, collective_id=0, has_side_effects=True),
        name="backward",
    )(hid, slope, x_in, x_mid, w_in_b, w_out_b, d_top, d_hid_top, extra)


SLOTS = 3


def update_kernel(
    rates, x_hbm, w_in, m_in, w_out, m_out, grads, images_all, w_head, m_head,
    new_w_in, new_m_in, new_w_out, new_m_out, new_w_head, new_m_head, next_logits,
    b_w_in, b_m_in, b_w_out, b_m_out, b_g_in, b_g_out, rows_all, tops, b_head, x, n, acc, pre, hid, w_in_b, w_out_b,
    load_sem, store_sem, x_sem, rows_sem, head_sem, *, tokens, image, tile, chunks, layers,
):
    rate, coef = rates[0], rates[1]
    steps = layers * chunks

    def place(step):
        layer, chunk = step // chunks, step % chunks
        cols = pl.ds(pl.multiple_of(chunk * CHUNK, CHUNK), CHUNK)
        return layer, chunk, cols, step % SLOTS

    def loads(step):
        layer, chunk, cols, slot = place(step)
        top = layer // (layers - 1)
        lower = (1 + 2 * (layers - 2 - layer) + chunk // 3) * 6 + 2 * (chunk % 3)
        block = top * chunk + (1 - top) * lower
        arrays = (
            (w_in.at[layer, :, cols], b_w_in),
            (m_in.at[layer, :, cols], b_m_in),
            (w_out.at[layer, cols, :], b_w_out),
            (m_out.at[layer, cols, :], b_m_out),
            (grads.at[block], b_g_in),
            (grads.at[block + 1 - top], b_g_out),
        )
        return [pltpu.make_async_copy(src, dst.at[slot], load_sem.at[slot, i]) for i, (src, dst) in enumerate(arrays)]

    def stores(step):
        layer, chunk, cols, slot = place(step)
        arrays = (
            (b_w_in, new_w_in.at[layer, :, cols]),
            (b_m_in, new_m_in.at[layer, :, cols]),
            (b_w_out, new_w_out.at[layer, cols, :]),
            (b_m_out, new_m_out.at[layer, cols, :]),
        )
        return [pltpu.make_async_copy(src.at[slot], dst, store_sem.at[slot, i]) for i, (src, dst) in enumerate(arrays)]

    load_x = pltpu.make_async_copy(x_hbm, x, x_sem)
    load_rows = pltpu.make_async_copy(images_all, rows_all, rows_sem)
    load_x.start()
    for ahead in range(SLOTS - 1):
        for load in loads(ahead):
            load.start()
    load_rows.start()
    head_loads = [pltpu.make_async_copy(src, b_head.at[i], head_sem.at[i]) for i, src in enumerate((w_head, m_head))]
    head_stores = [pltpu.make_async_copy(b_head.at[i], dst, head_sem.at[i]) for i, dst in enumerate((new_w_head, new_m_head))]
    for load in head_loads:
        load.start()
    load_x.wait()

    def start(rows):
        n[rows, :] = norm_rows(x[rows, :].astype(F32)).astype(BF16)
        acc[rows, :] = jnp.zeros_like(acc[rows, :])

    row_loop(tokens, 128, start)

    def per_image():
        load_rows.wait()
        for load in head_loads:
            load.wait()
        low = lax.broadcasted_iota(jnp.int32, (256, LANES), 0) % 8 >= 4
        for color in range(2):
            for third in range(3):
                value = rows_all[color, 6 + third].astype(F32)
                tops[color, third] = jnp.where(low, pltpu.roll(value, 4, 0), value).astype(BF16)
        classes = w_head.shape[0]
        for group in range(4):
            start = group * LANES
            size = min(LANES, classes - start)
            for third in range(3):
                at = (slice(start, start + size), span(third, LANES))
                grad = dot_lhs_t(rows_all[group // 2, 9 + group % 2], rows_all[group // 2, 6 + third])[:size]
                moment = coef * b_head[(1, *at)] + grad
                b_head[(1, *at)] = moment
                b_head[(0, *at)] = b_head[(0, *at)] - rate * moment
        for store in head_stores:
            store.start()

    @pl.loop(0, steps)
    def _(step):
        layer, chunk, _, slot = place(step)
        for load in loads(step):
            load.wait()

        for half in range(CHUNK // LANES):
            cols = span(half, LANES)
            moment = coef * b_m_in[slot, :, cols] + b_g_in[slot, span(half, b_w_in.shape[1]), :].astype(F32)
            weight = b_w_in[slot, :, cols] - rate * moment
            b_m_in[slot, :, cols] = moment
            b_w_in[slot, :, cols] = weight
            w_in_b[:, cols] = weight.astype(BF16)

        def update_out(grad_of):
            for third in range(768 // LANES):
                cols = span(third, LANES)
                moment = coef * b_m_out[slot, :, cols] + grad_of(third)
                weight = b_w_out[slot, :, cols] - rate * moment
                b_m_out[slot, :, cols] = moment
                b_w_out[slot, :, cols] = weight
                w_out_b[:, cols] = weight.astype(BF16)

        @pl.when(step == 2)
        def _():
            per_image()

        @pl.when(layer < layers - 1)
        def _():
            update_out(lambda third: b_g_out[slot, span(third, CHUNK), :].astype(F32))

        @pl.when(layer == layers - 1)
        def _():
            def top_grad(third):
                color = chunk // 3
                parts = [dot_lhs_t(rows_all[color, 2 * (chunk % 3) + half], tops[color, third]) for half in range(2)]
                return jnp.concatenate(parts, axis=0)

            update_out(top_grad)

        for store in stores(step):
            store.start()

        @pl.when(step >= 1)
        def _():
            for store in stores(step - 1):
                store.wait()

        @pl.when(step + SLOTS - 1 < steps)
        def _():
            for load in loads(step + SLOTS - 1):
                load.start()

        def first(i):
            pre[i % 2] = dot(n[span(i, tile), :], w_in_b[...])

        def act(i):
            for j in range(tile // ACT_ROWS):
                rows = span(j, ACT_ROWS)
                hid[i % 2, rows, :] = gelu_parts(pre[i % 2, rows, :])[-1].astype(BF16)

        def second(i):
            rows = span(i, tile)
            acc[rows, :] = dot(hid[i % 2], w_out_b[...]) + acc[rows, :]

        count = tokens // tile
        for i in range(count + 2):
            if i < count:
                first(i)
            if 0 <= i - 1 < count:
                act(i - 1)
            if i >= 2:
                second(i - 2)

        @pl.when(chunk == chunks - 1)
        def _():
            def finish(rows):
                value = (x[rows, :].astype(F32) + acc[rows, :]).astype(BF16)
                x[rows, :] = value
                n[rows, :] = norm_rows(value.astype(F32)).astype(BF16)
                acc[rows, :] = jnp.zeros_like(acc[rows, :])

            row_loop(tokens, 128, finish)

    pooled = (image_sums(x[...], image) / image).astype(BF16)
    next_logits[...] = dot_rhs_t(pooled, b_head[0].astype(BF16))
    for store in head_stores:
        store.wait()
    for store in stores(steps - 1):
        store.wait()


def update_and_next(rates, x, w_in, m_in, w_out, m_out, total, images_all, w_head, m_head, image=576):
    tokens, dim = x.shape
    layers, _, hidden = w_in.shape
    chunks = hidden // CHUNK
    tile = 384
    hbm = pl.BlockSpec(memory_space=pl.ANY)
    vmem = pl.BlockSpec(memory_space=pltpu.VMEM)
    dma = pltpu.SemaphoreType.DMA
    return pl.pallas_call(
        functools.partial(update_kernel, tokens=tokens, image=image, tile=tile, chunks=chunks, layers=layers),
        in_specs=[pl.BlockSpec(memory_space=pltpu.SMEM)] + [hbm] * 9,
        out_specs=[hbm] * 6 + [vmem],
        out_shape=[
            jax.ShapeDtypeStruct(w_in.shape, F32),
            jax.ShapeDtypeStruct(w_in.shape, F32),
            jax.ShapeDtypeStruct(w_out.shape, F32),
            jax.ShapeDtypeStruct(w_out.shape, F32),
            jax.ShapeDtypeStruct(w_head.shape, F32),
            jax.ShapeDtypeStruct(w_head.shape, F32),
            jax.ShapeDtypeStruct((8, w_head.shape[0]), F32),
        ],
        scratch_shapes=[
            pltpu.VMEM((SLOTS, dim, CHUNK), F32),
            pltpu.VMEM((SLOTS, dim, CHUNK), F32),
            pltpu.VMEM((SLOTS, CHUNK, dim), F32),
            pltpu.VMEM((SLOTS, CHUNK, dim), F32),
            pltpu.VMEM((SLOTS, 1536, LANES), BF16),
            pltpu.VMEM((SLOTS, 1536, LANES), BF16),
            pltpu.VMEM((2, GROUPS, 256, LANES), BF16),
            pltpu.VMEM((2, 3, 256, LANES), BF16),
            pltpu.VMEM((2, *w_head.shape), F32),
            pltpu.VMEM((tokens, dim), BF16),
            pltpu.VMEM((tokens, dim), BF16),
            pltpu.VMEM((tokens, dim), F32),
            pltpu.VMEM((2, tile, CHUNK), F32),
            pltpu.VMEM((2, tile, CHUNK), BF16),
            pltpu.VMEM((dim, CHUNK), BF16),
            pltpu.VMEM((CHUNK, dim), BF16),
            dma((SLOTS, 6)),
            dma((SLOTS, 4)),
            dma,
            dma,
            dma((2,)),
        ],
        compiler_params=pltpu.CompilerParams(vmem_limit_bytes=VMEM_LIMIT),
        name="update_next",
    )(rates, x, w_in, m_in, w_out, m_out, total.reshape(PAIRS * 6, 1536, LANES), images_all, w_head, m_head)


def solution(mesh):
    group_size = mesh.shape["data"]

    def local_step(x_step, labels, x_next, w_in, w_out, w_head, mom_in, mom_out, mom_head, learn_rate, mom_coef):
        micro, per_micro, image, dim = x_step.shape
        images = micro * per_micro
        layers, _, hidden = w_in.shape
        classes = w_head.shape[1]
        chunks = hidden // CHUNK
        examples = images * group_size
        w_head_b = w_head.astype(BF16)

        x_in = x_step.reshape(images * image, dim)
        hid, slope, w_in_b, w_out_b, x_mid, hid_sum, top_sum = forward(x_in, w_in, w_out, image)

        pooled = (top_sum[:images] / image).astype(BF16)
        soft_prob = jax.nn.softmax(dot(pooled, w_head_b), axis=-1)
        onehot = (labels.reshape(images, 1) == jnp.arange(classes)[None, :]).astype(F32)
        d_logits = ((soft_prob - onehot) / examples).astype(BF16)
        d_top = (dot_rhs_t(d_logits, w_head_b) / image).astype(BF16)
        d_hid_top = dot_rhs_t(d_top, w_out_b[layers - 1])
        d_hid_top = jnp.pad(d_hid_top, ((0, 8 - images), (0, 0))).reshape(8, chunks, CHUNK).transpose(1, 0, 2)

        hid_sum = hid_sum[:, :images].transpose(1, 0, 2).reshape(images, hidden)
        hid_high = lax.reduce_precision(hid_sum, 8, 7)
        hid_low = (hid_sum - hid_high).astype(BF16)
        wide = lambda a, b: jnp.concatenate([a, b]).reshape(2 * images, -1, LANES).transpose(1, 0, 2)
        logit_pad = jnp.pad(d_logits, ((0, 0), (0, 1024 - classes)))
        sums = wide(hid_high.astype(BF16), hid_low).reshape(2, -1, 2 * images, LANES)
        tops = jnp.broadcast_to(wide(d_top, pooled)[None], (2, 3, 2 * images, LANES))
        logit_rows = wide(jnp.zeros_like(logit_pad), logit_pad).reshape(2, -1, 2 * images, LANES)
        extra = jnp.concatenate([sums, tops, logit_rows], axis=1)

        total, images_all = backward(
            hid, slope, x_in, x_mid, w_in_b, w_out_b,
            jnp.pad(d_top.astype(F32), ((0, 8 - images), (0, 0))), d_hid_top, extra, image,
        )

        rates = jnp.stack([learn_rate, mom_coef])
        x_last = x_next.reshape(-1, dim)
        new_w_in, new_mom_in, new_w_out, new_mom_out, new_w_head, new_mom_head, logits_next = update_and_next(
            rates, x_last, w_in, mom_in, w_out, mom_out, total, images_all, w_head.T, mom_head.T, image
        )
        logits_next, new_w_head, new_mom_head = logits_next[: x_next.shape[0]], new_w_head.T, new_mom_head.T
        return (logits_next, new_w_in, new_w_out, new_w_head, new_mom_in, new_mom_out, new_mom_head)

    return jax.shard_map(
        local_step,
        mesh=mesh,
        in_specs=(P(None, "data", None, None), P(None, "data"), P("data", None, None), P(), P(), P(), P(), P(), P(), P(), P()),
        out_specs=(P("data", None), P(), P(), P(), P(), P(), P()),
        check_vma=False,
    )
```
